64 devices in a mesh: dp: 4 (over x, y), sp: 16 (over z, core).
Axes of the slice: x: 2, y: 2, z: 8, core: 2. Of those that a mesh axis runs over, the one named last changes fastest.
The devices are a block of a 4x4x8 slice.
Arguments:
- x: bfloat16 [16384, 2560], P(('dp', 'sp')), parts along dimension 0
- g_kv: bfloat16 [2560], replicated
- w_k: bfloat16 [2560, 20, 128], replicated
- w_v: bfloat16 [2560, 20, 128], replicated
- g_attn: bfloat16 [2, 2560], replicated
- w_q: bfloat16 [2, 2560, 20, 128], replicated
- w_o: bfloat16 [2, 20, 128, 2560], replicated
- g_mlp: bfloat16 [2, 2560], replicated
- w_gate: bfloat16 [2, 2560, 6912], replicated
- w_up: bfloat16 [2, 2560, 6912], replicated
- w_down: bfloat16 [2, 6912, 2560], replicated
Outputs:
- output: bfloat16 [16384, 2560], P(('dp', 'sp')), parts along dimension 0
There are 4 independent parts. The reference program is written for one: setup_inputs(seed, part) draws one part's arguments, and reference() takes and returns one part's arrays. A program takes and returns all parts, laid end to end along the dimension named above; an argument that names none is the same for every part.
All inputs are finite; a program needn't handle non-finite values.
Results may differ from the reference program's by a relative error of at most 0.0103382.
Values are sent between devices in bfloat16 or wider.
A program may use at most 768 MiB of HBM per device.

```python
import jax
import jax.numpy as jnp
from jax import lax

D = 2560
HEADS = 20
HEAD = 128
FF = 6912
LAYERS = 2
TOKENS_DEV = 256
SEQ_DEVS = 16
QUERY_BLOCK = 64
SEQ = SEQ_DEVS * TOKENS_DEV
WIDTH = HEADS * HEAD
EPS = 1e-6


def rms_norm(act_rows, gain_vec):
    act_f32 = act_rows.astype(jnp.float32)
    inv_rms = lax.rsqrt(jnp.mean(act_f32 * act_f32, axis=-1, keepdims=True) + EPS)
    return (act_f32 * inv_rms * gain_vec.astype(jnp.float32)).astype(jnp.bfloat16)


def setup_inputs(seed: int = 0, part: int = 0) -> dict:
    base_key = jax.random.key(seed)
    part_key = jax.random.fold_in(base_key, part)
    walk_key, noise_key = jax.random.split(part_key, 2)
    weight_keys = jax.random.split(base_key, 11)
    walk_steps = jax.random.normal(walk_key, (SEQ, D), jnp.float32) * (1.0 / SEQ) ** 0.5
    walk_sum = jnp.cumsum(walk_steps, axis=0)
    noise_rows = jax.random.normal(noise_key, (SEQ, D), jnp.float32)
    x = (walk_sum + 0.5 * noise_rows).astype(jnp.bfloat16)

    def normal_w(rand_key, arr_shape, fan_in, gain_mult):
        return (jax.random.normal(rand_key, arr_shape, jnp.float32) * (gain_mult * fan_in ** -0.5)).astype(jnp.bfloat16)

    def gain_w(rand_key, arr_shape):
        return (0.5 + jax.random.uniform(rand_key, arr_shape, jnp.float32)).astype(jnp.bfloat16)

    return {
        "x": x,
        "g_kv": gain_w(weight_keys[0], (D,)),
        "w_k": normal_w(weight_keys[1], (D, HEADS, HEAD), D, 1.0),
        "w_v": normal_w(weight_keys[2], (D, HEADS, HEAD), D, 1.0),
        "g_attn": gain_w(weight_keys[3], (LAYERS, D)),
        "w_q": normal_w(weight_keys[4], (LAYERS, D, HEADS, HEAD), D, 1.0),
        "w_o": normal_w(weight_keys[5], (LAYERS, HEADS, HEAD, D), WIDTH, 2.0),
        "g_mlp": gain_w(weight_keys[6], (LAYERS, D)),
        "w_gate": normal_w(weight_keys[7], (LAYERS, D, FF), D, 1.0),
        "w_up": normal_w(weight_keys[8], (LAYERS, D, FF), D, 1.0),
        "w_down": normal_w(weight_keys[9], (LAYERS, FF, D), FF, 1.0),
    }


def attend(queries, key_rows, value_rows):
    key_f32 = key_rows.astype(jnp.float32)
    value_f32 = value_rows.astype(jnp.float32)
    key_pos = jnp.arange(SEQ)

    def one_block(block_idx):
        start_row = block_idx * QUERY_BLOCK
        q_rows = lax.dynamic_slice_in_dim(queries, start_row, QUERY_BLOCK, axis=0).astype(jnp.float32)
        scores = jnp.einsum("qhe,khe->hqk", q_rows, key_f32) * HEAD ** -0.5
        query_pos = start_row + jnp.arange(QUERY_BLOCK)
        causal_mask = key_pos[None, :] <= query_pos[:, None]
        scores = jnp.where(causal_mask[None], scores, -jnp.inf)
        attn_probs = jax.nn.softmax(scores, axis=-1).astype(jnp.bfloat16)
        return jnp.einsum("hqk,khe->qhe", attn_probs.astype(jnp.float32), value_f32).astype(jnp.bfloat16)

    return lax.map(one_block, jnp.arange(SEQ // QUERY_BLOCK)).reshape(SEQ, WIDTH)


def reference(x, g_kv, w_k, w_v, g_attn, w_q, w_o, g_mlp, w_gate, w_up, w_down):
    normed = rms_norm(x, g_kv)
    key_rows = jnp.dot(normed, w_k.reshape(D, WIDTH), preferred_element_type=jnp.float32).astype(jnp.bfloat16).reshape(SEQ, HEADS, HEAD)
    value_rows = jnp.dot(normed, w_v.reshape(D, WIDTH), preferred_element_type=jnp.float32).astype(jnp.bfloat16).reshape(SEQ, HEADS, HEAD)

    def layer_step(hidden, layer_params):
        gain_attn, q_proj, out_proj, gain_mlp, gate_proj, up_proj, down_proj = layer_params
        normed_a = rms_norm(hidden, gain_attn)
        queries = jnp.dot(normed_a, q_proj.reshape(D, WIDTH), preferred_element_type=jnp.float32).astype(jnp.bfloat16).reshape(SEQ, HEADS, HEAD)
        attn_rows = attend(queries, key_rows, value_rows)
        hidden = (hidden.astype(jnp.float32) + jnp.dot(attn_rows, out_proj.reshape(WIDTH, D), preferred_element_type=jnp.float32)).astype(jnp.bfloat16)
        normed_m = rms_norm(hidden, gain_mlp)
        gate_act = jnp.dot(normed_m, gate_proj, preferred_element_type=jnp.float32)
        up_act = jnp.dot(normed_m, up_proj, preferred_element_type=jnp.float32)
        mixed = (jax.nn.silu(gate_act) * up_act).astype(jnp.bfloat16)
        hidden = (hidden.astype(jnp.float32) + jnp.dot(mixed, down_proj, preferred_element_type=jnp.float32)).astype(jnp.bfloat16)
        return hidden, None

    hidden, unused_out = lax.scan(layer_step, x, (g_attn, w_q, w_o, g_mlp, w_gate, w_up, w_down))
    return hidden
```

```python
import functools
import math

import jax
import jax.numpy as jnp
from jax import lax
from jax.experimental import pallas as pl
from jax.experimental.pallas import tpu as pltpu
from jax.sharding import PartitionSpec as P

EPS = 1e-6
LOG2E = 1.4426950408889634
MESH = pl.DeviceIdType.MESH
VMEM_LIMIT = 67043328
GROUP = 4


def norm_rows(src, gain, dst):
    rows = src.shape[0]
    step = math.gcd(rows, 32)
    g = gain[...].astype(jnp.float32)

    @pl.loop(0, rows // step)
    def _(i):
        sl = pl.ds(pl.multiple_of(i * step, step), step)
        v = src[sl, :].astype(jnp.float32)
        inv = lax.rsqrt(jnp.mean(v * v, axis=-1, keepdims=True) + EPS)
        dst[sl, :] = (v * inv * g).astype(jnp.bfloat16)


def heads_matrix(w):
    return jnp.concatenate([w[i] for i in range(GROUP)], axis=1)


def project(n, w):
    return jnp.dot(n, heads_matrix(w), preferred_element_type=jnp.float32).astype(jnp.bfloat16)


def attend_block(k_ref, v_ref, q_ref, m_ref, l_ref, acc_ref, unroll, mask=None):
    heads, _, head_dim = k_ref.shape
    scale = LOG2E * head_dim ** -0.5

    @pl.loop(0, heads // unroll)
    def _(g):
        hs = [g * unroll + i for i in range(unroll)]
        scores = [
            jnp.dot(k_ref[h], q_ref[h], preferred_element_type=jnp.float32) * scale
            for h in hs
        ]
        if mask is not None:
            scores = [jnp.where(mask, s, -jnp.inf) for s in scores]
        for h, s in zip(hs, scores):
            m_old = m_ref[h]
            m_new = jnp.maximum(m_old, jnp.max(s, axis=0, keepdims=True))
            alpha = jnp.exp2(m_old - m_new)
            p = jnp.exp2(s - m_new)
            m_ref[h] = m_new
            l_ref[h] = l_ref[h] * alpha + jnp.sum(p, axis=0, keepdims=True)
            acc_ref[h] = acc_ref[h] * alpha + jnp.dot(
                v_ref[h], p.astype(jnp.bfloat16), preferred_element_type=jnp.float32
            )


def reset_state(m_ref, l_ref, acc_ref):
    m_ref[...] = jnp.full_like(m_ref, -jnp.inf)
    l_ref[...] = jnp.zeros_like(l_ref)

    @pl.loop(0, acc_ref.shape[0])
    def _(h):
        acc_ref[h] = jnp.zeros(acc_ref.shape[1:], jnp.float32)


def write_attention(o_ref, l_ref, acc_ref):
    heads, head_dim, _ = acc_ref.shape

    for h in range(heads):
        o = acc_ref[h] / l_ref[h]
        o_ref[:, h * head_dim:(h + 1) * head_dim] = o.T.astype(jnp.bfloat16)


def causal_mask(tokens, half, core, d):
    shape = (2 * half, tokens)
    k = lax.broadcasted_iota(jnp.int32, shape, 0)
    q = lax.broadcasted_iota(jnp.int32, shape, 1)
    key_pos = jnp.where(k >= half, k - half + tokens, k) + d * half
    return key_pos <= q + core * tokens


def unit_valid(u, d, chip, chips):
    s = (u + 1) // 2
    return (chip >= s) if d == 0 else (chip + s >= chips)


def gather_attend_kernel(
    n_sp, x_hbm, g_kv, g_q, wk_hbm, wv_hbm, wq_hbm,
    k_all, v_all, o_ref,
    wk, wv, wq, xs, nb, kb, vb, ka, va, qt, m_ref, l_ref, acc,
    x_sem, w_sem, q_sem, send_sem, recv_sem, st_sem, px_sem, pr_sem, ld_sem,
):
    heads, depth, head_dim = wk.shape
    tokens = nb.shape[0]
    half = tokens // 2
    groups = heads // GROUP
    chips = n_sp // 2
    me = lax.axis_index("sp")
    chip = me // 2
    core = me - 2 * chip
    right = lax.rem(me + 2, n_sp)
    left = lax.rem(me + n_sp - 2, n_sp)
    partner = me + 1 - 2 * core

    barrier = pltpu.get_barrier_semaphore()
    for dev in (left, right, partner):
        pl.semaphore_signal(barrier, inc=1, device_id={"sp": dev}, device_id_type=MESH)
    pl.semaphore_wait(barrier, 3)

    def hop(src, u, d):
        return pltpu.make_async_remote_copy(
            src_ref=src,
            dst_ref=xs.at[u, pl.ds(d * half, half), :],
            send_sem=send_sem.at[u, d],
            recv_sem=recv_sem.at[u, d],
            device_id={"sp": right if d == 0 else left},
            device_id_type=MESH,
        )

    def own(u, d):
        return hop(x_hbm.at[pl.ds((u - 1) * half, half), :], u, d)

    def relay(u_from, u, d):
        return hop(xs.at[u_from, pl.ds(d * half, half), :], u, d)

    for u in (1, 2):
        for d in (0, 1):
            own(u, d).start()
    x_copy = pltpu.make_async_copy(x_hbm, xs.at[0], x_sem)
    x_copy.start()

    def w_copy(which, j):
        src, dst = ((wk_hbm, wk), (wv_hbm, wv))[which]
        sl = pl.ds(j * GROUP, GROUP)
        return pltpu.make_async_copy(src.at[sl], dst.at[sl], w_sem.at[which, j])

    def q_copy(j, slot):
        return pltpu.make_async_copy(
            wq_hbm.at[0, pl.ds(j * GROUP, GROUP)], wq.at[slot], q_sem.at[slot])

    for j in range(groups):
        w_copy(0, j).start()
        w_copy(1, j).start()
    for j in range(min(2, groups)):
        q_copy(j, j).start()
    reset_state(m_ref, l_ref, acc)
    x_copy.wait()

    def stores(u, slot):
        out = []
        for i, (buf, full) in enumerate(((kb, k_all), (vb, v_all))):
            for d in (0, 1):
                part = pl.ds(d * half, half)
                mine = pl.ds(core * half, half)
                if i == 0:
                    src, dst = buf.at[slot, :, part, :], full.at[u, d, :, mine, :]
                else:
                    src, dst = buf.at[slot, :, :, part], full.at[u, d, :, :, mine]
                local = pltpu.make_async_copy(src, dst, st_sem.at[slot, i, d])
                remote = pltpu.make_async_remote_copy(
                    src_ref=src, dst_ref=dst,
                    send_sem=px_sem.at[slot, i, d], recv_sem=pr_sem.at[u, i, d],
                    device_id={"sp": partner}, device_id_type=MESH,
                )
                out.append((local, remote))
        return out

    def loads(u, d):
        return (
            pltpu.make_async_copy(k_all.at[u, d], ka.at[d], ld_sem.at[d, 0]),
            pltpu.make_async_copy(v_all.at[u, d], va.at[d], ld_sem.at[d, 1]),
        )

    def finish_stores(u):
        for local, remote in stores(u, lax.rem(u, 2)):
            local.wait()
            remote.wait_send()
            remote.wait_recv()

    def attend_unit(u):
        for d in (0, 1):
            for copy in loads(u, d):
                copy.wait()

            @pl.when(unit_valid(u, d, chip, chips))
            def _():
                attend_block(ka.at[d], va.at[d], qt, m_ref, l_ref, acc, 4)

    def attend_own():
        for d in (0, 1):
            for copy in loads(0, d):
                copy.wait()
            attend_block(ka.at[d], va.at[d], qt, m_ref, l_ref, acc, 2,
                         mask=causal_mask(tokens, half, core, d))

    @pl.loop(0, chips)
    def _(u):
        slot = lax.rem(u, 2)

        @pl.when(u >= 1)
        def _():
            for d in (0, 1):
                relay(0, u, d).wait_recv()

        @pl.when(jnp.logical_and(u >= 1, u <= chips - 4))
        def _():
            for d in (0, 1):
                relay(u, u + 2, d).start()

        @pl.when(u == chips - 3)
        def _():
            relay(u, u + 2, 0).start()

        @pl.when(u == chips - 2)
        def _():
            relay(u, u + 1, 1).start()

        @pl.when(u >= 1)
        def _():
            finish_stores(u - 1)
            for d in (0, 1):
                for copy in loads(u - 1, d):
                    copy.start()

        norm_rows(xs.at[u], g_kv, nb)

        @pl.loop(0, groups)
        def _(j):
            @pl.when(u == 0)
            def _():
                w_copy(0, j).wait()
                w_copy(1, j).wait()

            sl = pl.ds(j * GROUP, GROUP)
            n = nb[...]
            k = project(n, wk[sl])
            v = project(n, wv[sl])
            for i in range(GROUP):
                cols = slice(i * head_dim, (i + 1) * head_dim)
                kb[slot, j * GROUP + i] = k[:, cols]
                vb[slot, j * GROUP + i] = v[:, cols].T

        for local, remote in stores(u, slot):
            local.start()
            remote.start()

        @pl.when(u == 0)
        def _():
            norm_rows(xs.at[0], g_q, nb)

            @pl.loop(0, groups)
            def _(j):
                qslot = lax.rem(j, 2)
                q_copy(j, qslot).wait()
                q = project(nb[...], wq[qslot])
                for i in range(GROUP):
                    qt[j * GROUP + i] = q[:, i * head_dim:(i + 1) * head_dim].T

                @pl.when(j + 2 < groups)
                def _():
                    q_copy(j + 2, qslot).start()

        @pl.when(u == 1)
        def _():
            attend_own()

        @pl.when(u >= 2)
        def _():
            attend_unit(u - 1)

    last = chips - 1
    finish_stores(last)
    for d in (0, 1):
        for copy in loads(last, d):
            copy.start()
    attend_unit(last)
    write_attention(o_ref, l_ref, acc)
    for u in range(1, chips):
        for d in (0, 1):
            relay(0, u, d).wait_send()


def gather_attend(n_sp, x, g_kv, g_q, wk, wv, wq):
    tokens, depth = x.shape
    heads, _, head_dim = wk.shape
    chips = n_sp // 2
    bf, f32 = jnp.bfloat16, jnp.float32
    dma = pltpu.SemaphoreType.DMA
    groups = heads // GROUP
    any_spec = pl.BlockSpec(memory_space=pl.ANY)
    vmem = pl.BlockSpec(memory_space=pltpu.VMEM)
    return pl.pallas_call(
        functools.partial(gather_attend_kernel, n_sp),
        out_shape=(
            jax.ShapeDtypeStruct((chips, 2, heads, tokens, head_dim), bf),
            jax.ShapeDtypeStruct((chips, 2, heads, head_dim, tokens), bf),
            jax.ShapeDtypeStruct((tokens, heads * head_dim), bf),
        ),
        in_specs=[any_spec, vmem, vmem, any_spec, any_spec, any_spec],
        out_specs=(any_spec, any_spec, vmem),
        scratch_shapes=[
            pltpu.VMEM((heads, depth, head_dim), bf),
            pltpu.VMEM((heads, depth, head_dim), bf),
            pltpu.VMEM((2, GROUP, depth, head_dim), bf),
            pltpu.VMEM((chips, tokens, depth), bf),
            pltpu.VMEM((tokens, depth), bf),
            pltpu.VMEM((2, heads, tokens, head_dim), bf),
            pltpu.VMEM((2, heads, head_dim, tokens), bf),
            pltpu.VMEM((2, heads, tokens, head_dim), bf),
            pltpu.VMEM((2, heads, head_dim, tokens), bf),
            pltpu.VMEM((heads, head_dim, tokens), bf),
            pltpu.VMEM((heads, 1, tokens), f32),
            pltpu.VMEM((heads, 1, tokens), f32),
            pltpu.VMEM((heads, head_dim, tokens), f32),
            dma,
            dma((2, groups)),
            dma((2,)),
            dma((chips, 2)),
            dma((chips, 2)),
            dma((2, 2, 2)),
            dma((2, 2, 2)),
            dma((chips, 2, 2)),
            dma((2, 2)),
        ],
        compiler_params=pltpu.CompilerParams(
            collective_id=0, has_side_effects=True, vmem_limit_bytes=VMEM_LIMIT
        ),
        name="gather_attend",
    )(x, g_kv, g_q, wk, wv, wq)


def attend_kernel(
    n_sp, layer, h_ref, g_q, wq_hbm, k_all, v_all, o_ref,
    wq, nb, ka, va, qt, m_ref, l_ref, acc, q_sem, ld_sem,
):
    heads, head_dim, tokens = qt.shape
    half = tokens // 2
    groups = heads // GROUP
    chips = n_sp // 2
    bufs = ka.shape[0]
    me = lax.axis_index("sp")
    chip = me // 2
    core = me - 2 * chip

    def q_copy(j, slot):
        return pltpu.make_async_copy(
            wq_hbm.at[layer, pl.ds(j * GROUP, GROUP)], wq.at[slot], q_sem.at[slot])

    def loads(u, d, slot):
        return (
            pltpu.make_async_copy(k_all.at[u, d], ka.at[slot], ld_sem.at[slot, 0]),
            pltpu.make_async_copy(v_all.at[u, d], va.at[slot], ld_sem.at[slot, 1]),
        )

    for j in range(min(2, groups)):
        q_copy(j, j).start()
    for i in range(bufs):
        for copy in loads(i // 2, i % 2, i):
            copy.start()
    reset_state(m_ref, l_ref, acc)
    norm_rows(h_ref, g_q, nb)

    @pl.loop(0, groups)
    def _(j):
        qslot = lax.rem(j, 2)
        q_copy(j, qslot).wait()
        q = project(nb[...], wq[qslot])
        for i in range(GROUP):
            qt[j * GROUP + i] = q[:, i * head_dim:(i + 1) * head_dim].T

        @pl.when(j + 2 < groups)
        def _():
            q_copy(j + 2, qslot).start()

    @pl.loop(0, chips)
    def _(u):
        for d in (0, 1):
            slot = lax.rem(2 * u + d, bufs)
            for copy in loads(u, d, slot):
                copy.wait()

            @pl.when(u == 0)
            def _():
                attend_block(ka.at[slot], va.at[slot], qt, m_ref, l_ref, acc, 2,
                             mask=causal_mask(tokens, half, core, d))

            @pl.when(jnp.logical_and(u > 0, unit_valid(u, d, chip, chips)))
            def _():
                attend_block(ka.at[slot], va.at[slot], qt, m_ref, l_ref, acc, 4)

            nxt = 2 * u + d + bufs

            @pl.when(nxt < 2 * chips)
            def _():
                for copy in loads(nxt // 2, lax.rem(nxt, 2), slot):
                    copy.start()

    write_attention(o_ref, l_ref, acc)


def attend(n_sp, layer, h, g_q, wq, k_all, v_all):
    tokens, depth = h.shape
    _, heads, _, head_dim = wq.shape
    bf, f32 = jnp.bfloat16, jnp.float32
    dma = pltpu.SemaphoreType.DMA
    bufs = 4
    any_spec = pl.BlockSpec(memory_space=pl.ANY)
    vmem = pl.BlockSpec(memory_space=pltpu.VMEM)
    return pl.pallas_call(
        functools.partial(attend_kernel, n_sp, layer),
        out_shape=jax.ShapeDtypeStruct((tokens, heads * head_dim), bf),
        in_specs=[vmem, vmem, any_spec, any_spec, any_spec],
        out_specs=vmem,
        scratch_shapes=[
            pltpu.VMEM((2, GROUP, depth, head_dim), bf),
            pltpu.VMEM((tokens, depth), bf),
            pltpu.VMEM((bufs, heads, tokens, head_dim), bf),
            pltpu.VMEM((bufs, heads, head_dim, tokens), bf),
            pltpu.VMEM((heads, head_dim, tokens), bf),
            pltpu.VMEM((heads, 1, tokens), f32),
            pltpu.VMEM((heads, 1, tokens), f32),
            pltpu.VMEM((heads, head_dim, tokens), f32),
            dma((2,)),
            dma((bufs, 2)),
        ],
        compiler_params=pltpu.CompilerParams(vmem_limit_bytes=VMEM_LIMIT),
        name="attend",
    )(h, g_q, wq, k_all, v_all)


def tail_kernel(
    layer, o_ref, h_ref, g_ref, wo_hbm, wg_hbm, wu_hbm, wd_hbm, out_ref,
    wo, wg, wu, wd, hm, nb, acc, mb, o_sem, w_sem,
):
    tokens, depth = h_ref.shape
    parts, _, o_cols = wo.shape
    bufs, _, cols = wg.shape
    steps = wg_hbm.shape[2] // cols
    sub = math.gcd(cols, 256)
    span = math.gcd(depth, 512)

    def o_copy(j):
        return pltpu.make_async_copy(
            wo_hbm.at[layer, :, pl.ds(j * o_cols, o_cols)], wo.at[j], o_sem.at[j])

    def w_copies(i, slot):
        sl = pl.ds(pl.multiple_of(i * cols, cols), cols)
        return (
            pltpu.make_async_copy(wg_hbm.at[layer, :, sl], wg.at[slot], w_sem.at[slot, 0]),
            pltpu.make_async_copy(wu_hbm.at[layer, :, sl], wu.at[slot], w_sem.at[slot, 1]),
            pltpu.make_async_copy(wd_hbm.at[layer, sl, :], wd.at[slot], w_sem.at[slot, 2]),
        )

    for j in range(parts):
        o_copy(j).start()
    for i in range(min(bufs, steps)):
        for copy in w_copies(i, i):
            copy.start()

    for j in range(parts):
        o_copy(j).wait()
        sl = slice(j * o_cols, (j + 1) * o_cols)
        r = jnp.dot(o_ref[...], wo[j], preferred_element_type=jnp.float32)
        h = (h_ref[:, sl].astype(jnp.float32) + r).astype(jnp.bfloat16)
        hm[:, sl] = h
        acc[:, sl] = h.astype(jnp.float32)
    norm_rows(hm, g_ref, nb)

    @pl.loop(0, steps)
    def _(i):
        slot = lax.rem(i, bufs)
        for copy in w_copies(i, slot):
            copy.wait()
        n = nb[...]
        for s in range(cols // sub):
            sl = slice(s * sub, (s + 1) * sub)
            a = jnp.dot(n, wg[slot, :, sl], preferred_element_type=jnp.float32)
            b = jnp.dot(n, wu[slot, :, sl], preferred_element_type=jnp.float32)
            mb[:, sl] = (jax.nn.silu(a) * b).astype(jnp.bfloat16)
        m = mb[...]
        for t in range(depth // span):
            sl = slice(t * span, (t + 1) * span)
            acc[:, sl] += jnp.dot(m, wd[slot, :, sl], preferred_element_type=jnp.float32)

        @pl.when(i + bufs < steps)
        def _():
            for copy in w_copies(i + bufs, slot):
                copy.start()

    out_ref[...] = acc[...].astype(jnp.bfloat16)


def tail(layer, o, h, g, wo, wg, wu, wd):
    tokens, depth = h.shape
    ff = wg.shape[2]
    bf, f32 = jnp.bfloat16, jnp.float32
    dma = pltpu.SemaphoreType.DMA
    bufs = 3
    cols = math.gcd(ff, 768)
    o_cols = math.gcd(depth, 512)
    parts = depth // o_cols
    any_spec = pl.BlockSpec(memory_space=pl.ANY)
    vmem = pl.BlockSpec(memory_space=pltpu.VMEM)
    return pl.pallas_call(
        functools.partial(tail_kernel, layer),
        out_shape=jax.ShapeDtypeStruct((tokens, depth), bf),
        in_specs=[vmem, vmem, vmem] + [any_spec] * 4,
        out_specs=vmem,
        scratch_shapes=[
            pltpu.VMEM((parts, wo.shape[1], o_cols), bf),
            pltpu.VMEM((bufs, depth, cols), bf),
            pltpu.VMEM((bufs, depth, cols), bf),
            pltpu.VMEM((bufs, cols, depth), bf),
            pltpu.VMEM((tokens, depth), bf),
            pltpu.VMEM((tokens, depth), bf),
            pltpu.VMEM((tokens, depth), f32),
            pltpu.VMEM((tokens, cols), bf),
            dma((parts,)),
            dma((bufs, 3)),
        ],
        compiler_params=pltpu.CompilerParams(vmem_limit_bytes=VMEM_LIMIT),
        name="tail",
    )(o, h, g, wo, wg, wu, wd)


def solution(mesh):
    n_sp = mesh.shape["sp"]
    row_spec = P(("dp", "sp"), None)
    in_specs = (row_spec,) + (P(),) * 10

    def local_block(x, g_kv, w_k, w_v, g_attn, w_q, w_o, g_mlp, w_gate, w_up, w_down):
        depth = x.shape[1]
        wk = w_k.transpose(1, 0, 2)
        wv = w_v.transpose(1, 0, 2)
        wq = w_q.transpose(0, 2, 1, 3)
        wo = w_o.reshape(w_o.shape[0], -1, depth)
        k_all, v_all, o = gather_attend(
            n_sp, x, g_kv.reshape(1, -1), g_attn[0:1], wk, wv, wq)
        h = tail(0, o, x, g_mlp[0:1], wo, w_gate, w_up, w_down)
        for layer in range(1, w_q.shape[0]):
            o = attend(n_sp, layer, h, g_attn[layer:layer + 1], wq, k_all, v_all)
            h = tail(layer, o, h, g_mlp[layer:layer + 1], wo, w_gate, w_up, w_down)
        return h

    return jax.shard_map(local_block, mesh=mesh, in_specs=in_specs, out_specs=row_spec, check_vma=False)
```

```python
import functools
import math

import jax
import jax.numpy as jnp
from jax import lax
from jax.experimental import pallas as pl
from jax.experimental.pallas import tpu as pltpu
from jax.sharding import PartitionSpec as P

EPS = 1e-6
LOG2E = 1.4426950408889634
MESH = pl.DeviceIdType.MESH
VMEM_LIMIT = 67043328
GROUP = 4
UNROLL = 4


def norm_rows(src, gain, dst):
    rows = src.shape[0]
    step = math.gcd(rows, 16)
    g = gain.astype(jnp.float32)

    def body(i, carry):
        sl = pl.ds(pl.multiple_of(i * step, step), step)
        v = src[sl, :].astype(jnp.float32)
        inv = lax.rsqrt(jnp.mean(v * v, axis=-1, keepdims=True) + EPS)
        dst[sl, :] = (v * inv * g).astype(jnp.bfloat16)
        return carry

    lax.fori_loop(0, rows // step, body, 0, unroll=4)


def heads_matrix(w):
    return jnp.concatenate([w[i] for i in range(GROUP)], axis=1)


def project(n, w):
    return jnp.dot(n, heads_matrix(w), preferred_element_type=jnp.float32).astype(jnp.bfloat16)


def all_sublanes(x, op):
    for shift in (4, 2, 1):
        x = op(x, pltpu.roll(x, shift, 0))
    return x


def attend_block(ks, vs, q_ref, m_ref, l_ref, acc_ref, s_refs, masks=None):
    heads, size, head_dim = ks[0].shape
    tokens = q_ref.shape[2]
    scale = LOG2E * head_dim ** -0.5
    n = size // 8

    def scores(h, s_ref):
        top = None
        for i, k in enumerate(ks):
            s = jnp.dot(k[h], q_ref[h], preferred_element_type=jnp.float32)
            if masks is not None:
                s = jnp.where(masks[i], s, -jnp.inf)
            s = s.reshape(n, 8, tokens)
            s_ref[i * n:(i + 1) * n] = s
            t = jnp.max(s, axis=0)
            top = t if top is None else jnp.maximum(top, t)
        return all_sublanes(top, jnp.maximum)

    def update(h, s_ref, top):
        m_old = m_ref[h]
        m_new = jnp.maximum(m_old, top * scale)
        alpha = jnp.exp2(m_old - m_new)
        m_ref[h] = m_new
        p = jnp.exp2(s_ref[:n * len(ks)] * scale - m_new[None])
        l_ref[h] = l_ref[h] * alpha + jnp.sum(p, axis=0)
        p = p.reshape(size * len(ks), tokens).astype(jnp.bfloat16)
        v = jnp.concatenate([r[h] for r in vs], axis=1) if len(vs) > 1 else vs[0][h]
        o = jnp.dot(v, p, preferred_element_type=jnp.float32)
        acc_ref[h] = acc_ref[h] * alpha[None] + o.reshape(head_dim // 8, 8, tokens)

    def body(g, top):
        h = UNROLL * g
        for i in range(UNROLL):
            nxt = h + i + 1
            if i == UNROLL - 1:
                nxt = jnp.minimum(nxt, heads - 1)
            after = scores(nxt, s_refs[(i + 1) % 2])
            update(h + i, s_refs[i % 2], top)
            top = after
        return top

    lax.fori_loop(0, heads // UNROLL, body, scores(0, s_refs[0]))


def reset_state(m_ref, l_ref, acc_ref):
    m_ref[...] = jnp.full_like(m_ref, -jnp.inf)
    l_ref[...] = jnp.zeros_like(l_ref)

    @pl.loop(0, acc_ref.shape[0])
    def _(h):
        acc_ref[h] = jnp.zeros(acc_ref.shape[1:], jnp.float32)


def write_attention(o_ref, l_ref, acc_ref):
    heads, _, _, tokens = acc_ref.shape
    head_dim = o_ref.shape[1] // heads

    @pl.loop(0, heads)
    def _(h):
        inv = 1.0 / all_sublanes(l_ref[h], jnp.add)
        o = (acc_ref[h] * inv[None]).reshape(head_dim, tokens)
        cols = pl.ds(pl.multiple_of(h * head_dim, head_dim), head_dim)
        o_ref[:, cols] = o.astype(jnp.bfloat16).T


def causal_mask(tokens, half, core, d):
    shape = (2 * half, tokens)
    k = lax.broadcasted_iota(jnp.int32, shape, 0)
    q = lax.broadcasted_iota(jnp.int32, shape, 1)
    key_pos = jnp.where(k >= half, k - half + tokens, k) + d * half
    return key_pos <= q + core * tokens


def attend_valid(u, chip, chips, ks, vs, state):
    s = (u + 1) // 2

    @pl.when(chip + s >= chips)
    def _():
        attend_block(ks, vs, *state)

    @pl.when(jnp.logical_and(chip >= s, chip + s < chips))
    def _():
        attend_block(ks[:1], vs[:1], *state)


def gather_attend_kernel(
    n_sp, x_hbm, g_kv, g_q, wk_hbm, wv_hbm, wq_hbm,
    k_all, v_all, o_ref,
    wk, wv, wq, xs, nb, kb, vb, ka, va, qt, m_ref, l_ref, acc, s0, s1,
    x_sem, w_sem, q_sem, send_sem, recv_sem, st_sem, px_sem, pr_sem, ld_sem,
):
    heads, depth, head_dim = wk.shape
    tokens = nb.shape[0]
    half = tokens // 2
    groups = heads // GROUP
    chips = n_sp // 2
    me = lax.axis_index("sp")
    chip = me // 2
    core = me - 2 * chip
    right = lax.rem(me + 2, n_sp)
    left = lax.rem(me + n_sp - 2, n_sp)
    partner = me + 1 - 2 * core

    barrier = pltpu.get_barrier_semaphore()
    for dev in (left, right, partner):
        pl.semaphore_signal(barrier, inc=1, device_id={"sp": dev}, device_id_type=MESH)
    pl.semaphore_wait(barrier, 3)

    def hop(src, u, d):
        return pltpu.make_async_remote_copy(
            src_ref=src,
            dst_ref=xs.at[u, pl.ds(d * half, half), :],
            send_sem=send_sem.at[u, d],
            recv_sem=recv_sem.at[u, d],
            device_id={"sp": right if d == 0 else left},
            device_id_type=MESH,
        )

    def own(u, d):
        return hop(x_hbm.at[pl.ds((u - 1) * half, half), :], u, d)

    def relay(u_from, u, d):
        return hop(xs.at[u_from, pl.ds(d * half, half), :], u, d)

    for u in (1, 2):
        for d in (0, 1):
            own(u, d).start()
    x_copy = pltpu.make_async_copy(x_hbm, xs.at[0], x_sem)
    x_copy.start()

    def w_copy(which, j):
        src, dst = ((wk_hbm, wk), (wv_hbm, wv))[which]
        sl = pl.ds(j * GROUP, GROUP)
        return pltpu.make_async_copy(src.at[sl], dst.at[sl], w_sem.at[which, j])

    def q_copy(j, slot):
        return pltpu.make_async_copy(
            wq_hbm.at[0, pl.ds(j * GROUP, GROUP)], wq.at[slot], q_sem.at[slot])

    ahead = min(2, groups)
    for j in range(ahead):
        w_copy(0, j).start()
        w_copy(1, j).start()
    reset_state(m_ref, l_ref, acc)
    x_copy.wait()

    def stores(u, slot, j):
        out = []
        hs = pl.ds(j * GROUP, GROUP)
        for i, (buf, full) in enumerate(((kb, k_all), (vb, v_all))):
            for d in (0, 1):
                part = pl.ds(d * half, half)
                mine = pl.ds(core * half, half)
                if i == 0:
                    src, dst = buf.at[slot, hs, part, :], full.at[u, d, hs, mine, :]
                else:
                    src, dst = buf.at[slot, hs, :, part], full.at[u, d, hs, :, mine]
                local = pltpu.make_async_copy(src, dst, st_sem.at[slot, j, i, d])
                remote = pltpu.make_async_remote_copy(
                    src_ref=src, dst_ref=dst,
                    send_sem=px_sem.at[slot, j, i, d], recv_sem=pr_sem.at[u, j, i, d],
                    device_id={"sp": partner}, device_id_type=MESH,
                )
                out.append((local, remote))
        return out

    def loads(u):
        out = []
        for d in (0, 1):
            out.append(pltpu.make_async_copy(k_all.at[u, d], ka.at[d], ld_sem.at[d, 0]))
            out.append(pltpu.make_async_copy(v_all.at[u, d], va.at[d], ld_sem.at[d, 1]))
        return out

    def finish_stores(u):
        @pl.loop(0, groups)
        def _(j):
            for local, remote in stores(u, lax.rem(u, 2), j):
                local.wait()
                remote.wait_send()
                remote.wait_recv()

    state = (qt, m_ref, l_ref, acc, (s0, s1))

    def attend_unit(u):
        for copy in loads(u):
            copy.wait()
        attend_valid(u, chip, chips, [ka.at[0], ka.at[1]], [va.at[0], va.at[1]], state)

    def attend_own():
        for copy in loads(0):
            copy.wait()
        masks = [causal_mask(tokens, half, core, d) for d in (0, 1)]
        attend_block([ka.at[0], ka.at[1]], [va.at[0], va.at[1]], *state, masks=masks)

    @pl.loop(0, chips)
    def _(u):
        slot = lax.rem(u, 2)

        @pl.when(u >= 1)
        def _():
            for d in (0, 1):
                relay(0, u, d).wait_recv()

        @pl.when(jnp.logical_and(u >= 1, u <= chips - 4))
        def _():
            for d in (0, 1):
                relay(u, u + 2, d).start()

        @pl.when(u == chips - 3)
        def _():
            relay(u, u + 2, 0).start()

        @pl.when(u == chips - 2)
        def _():
            relay(u, u + 1, 1).start()

        @pl.when(u >= 1)
        def _():
            finish_stores(u - 1)
            for copy in loads(u - 1):
                copy.start()

        norm_rows(xs.at[u], g_kv[...].reshape(1, depth), nb)

        @pl.loop(0, groups)
        def _(j):
            @pl.when(u == 0)
            def _():
                w_copy(0, j).wait()
                w_copy(1, j).wait()

                @pl.when(j + ahead < groups)
                def _():
                    w_copy(0, j + ahead).start()
                    w_copy(1, j + ahead).start()

                @pl.when(j + ahead >= groups)
                def _():
                    q_copy(j + ahead - groups, j + ahead - groups).start()

            sl = pl.ds(j * GROUP, GROUP)
            n = nb[...]
            k = project(n, wk[sl])
            v = project(n, wv[sl])
            for i in range(GROUP):
                cols = slice(i * head_dim, (i + 1) * head_dim)
                kb[slot, j * GROUP + i] = k[:, cols]
                vb[slot, j * GROUP + i] = v[:, cols].T
            for local, remote in stores(u, slot, j):
                local.start()
                remote.start()

        @pl.when(u == 0)
        def _():
            norm_rows(xs.at[0], g_q[0:1, :], nb)

            @pl.loop(0, groups)
            def _(j):
                qslot = lax.rem(j, 2)
                q_copy(j, qslot).wait()
                q = project(nb[...], wq[qslot])
                for i in range(GROUP):
                    qt[j * GROUP + i] = q[:, i * head_dim:(i + 1) * head_dim].T

                @pl.when(j + 2 < groups)
                def _():
                    q_copy(j + 2, qslot).start()

        @pl.when(u == 1)
        def _():
            attend_own()

        @pl.when(u >= 2)
        def _():
            attend_unit(u - 1)

    last = chips - 1
    finish_stores(last)
    for copy in loads(last):
        copy.start()
    attend_unit(last)
    write_attention(o_ref, l_ref, acc)
    for u in range(1, chips):
        for d in (0, 1):
            relay(0, u, d).wait_send()


def gather_attend(n_sp, x, g_kv, g_q, wk, wv, wq):
    tokens, depth = x.shape
    heads, _, head_dim = wk.shape
    chips = n_sp // 2
    bf, f32 = jnp.bfloat16, jnp.float32
    dma = pltpu.SemaphoreType.DMA
    groups = heads // GROUP
    any_spec = pl.BlockSpec(memory_space=pl.ANY)
    vmem = pl.BlockSpec(memory_space=pltpu.VMEM)
    return pl.pallas_call(
        functools.partial(gather_attend_kernel, n_sp),
        out_shape=(
            jax.ShapeDtypeStruct((chips, 2, heads, tokens, head_dim), bf),
            jax.ShapeDtypeStruct((chips, 2, heads, head_dim, tokens), bf),
            jax.ShapeDtypeStruct((tokens, heads * head_dim), bf),
        ),
        in_specs=[any_spec, vmem, vmem, any_spec, any_spec, any_spec],
        out_specs=(any_spec, any_spec, vmem),
        scratch_shapes=[
            pltpu.VMEM((heads, depth, head_dim), bf),
            pltpu.VMEM((heads, depth, head_dim), bf),
            pltpu.VMEM((2, GROUP, depth, head_dim), bf),
            pltpu.VMEM((chips, tokens, depth), bf),
            pltpu.VMEM((tokens, depth), bf),
            pltpu.VMEM((2, heads, tokens, head_dim), bf),
            pltpu.VMEM((2, heads, head_dim, tokens), bf),
            pltpu.VMEM((2, heads, tokens, head_dim), bf),
            pltpu.VMEM((2, heads, head_dim, tokens), bf),
            pltpu.VMEM((heads, head_dim, tokens), bf),
            pltpu.VMEM((heads, 8, tokens), f32),
            pltpu.VMEM((heads, 8, tokens), f32),
            pltpu.VMEM((heads, head_dim // 8, 8, tokens), f32),
            pltpu.VMEM((tokens // 4, 8, tokens), f32),
            pltpu.VMEM((tokens // 4, 8, tokens), f32),
            dma,
            dma((2, groups)),
            dma((2,)),
            dma((chips, 2)),
            dma((chips, 2)),
            dma((2, groups, 2, 2)),
            dma((2, groups, 2, 2)),
            dma((chips, groups, 2, 2)),
            dma((2, 2)),
        ],
        compiler_params=pltpu.CompilerParams(
            collective_id=0, has_side_effects=True, vmem_limit_bytes=VMEM_LIMIT
        ),
        name="gather_attend",
    )(x, g_kv, g_q, wk, wv, wq)


def attend_kernel(
    n_sp, layer, h_ref, g_q, wq_hbm, k_all, v_all, o_ref,
    wq, nb, ka, va, qt, m_ref, l_ref, acc, s0, s1, q_sem, ld_sem,
):
    heads, head_dim, tokens = qt.shape
    half = tokens // 2
    groups = heads // GROUP
    chips = n_sp // 2
    bufs = ka.shape[0]
    q_bufs = wq.shape[0]
    me = lax.axis_index("sp")
    chip = me // 2
    core = me - 2 * chip

    def q_copy(j, slot):
        return pltpu.make_async_copy(
            wq_hbm.at[layer, pl.ds(j * GROUP, GROUP)], wq.at[slot], q_sem.at[slot])

    def loads(u, slot):
        return (
            pltpu.make_async_copy(k_all.at[u], ka.at[slot], ld_sem.at[slot, 0]),
            pltpu.make_async_copy(v_all.at[u], va.at[slot], ld_sem.at[slot, 1]),
        )

    for j in range(min(q_bufs, groups)):
        q_copy(j, j).start()
    reset_state(m_ref, l_ref, acc)
    norm_rows(h_ref, g_q[layer:layer + 1, :], nb)

    @pl.loop(0, groups)
    def _(j):
        qslot = lax.rem(j, q_bufs)
        q_copy(j, qslot).wait()

        @pl.when(j >= groups - min(bufs - 1, groups))
        def _():
            i = j - (groups - min(bufs - 1, groups))
            for copy in loads(i, i):
                copy.start()

        q = project(nb[...], wq[qslot])
        for i in range(GROUP):
            qt[j * GROUP + i] = q[:, i * head_dim:(i + 1) * head_dim].T

        @pl.when(j + q_bufs < groups)
        def _():
            q_copy(j + q_bufs, qslot).start()

    for i in range(min(bufs - 1, groups), bufs - 1):
        for copy in loads(i, i):
            copy.start()

    state = (qt, m_ref, l_ref, acc, (s0, s1))

    @pl.loop(0, chips)
    def _(u):
        slot = lax.rem(u, bufs)
        for copy in loads(u, slot):
            copy.wait()
        ahead = u + bufs - 1

        @pl.when(ahead < chips)
        def _():
            for copy in loads(ahead, lax.rem(ahead, bufs)):
                copy.start()

        ks = [ka.at[slot, d] for d in (0, 1)]
        vs = [va.at[slot, d] for d in (0, 1)]

        @pl.when(u == 0)
        def _():
            masks = [causal_mask(tokens, half, core, d) for d in (0, 1)]
            attend_block(ks, vs, *state, masks=masks)

        @pl.when(u > 0)
        def _():
            attend_valid(u, chip, chips, ks, vs, state)

    write_attention(o_ref, l_ref, acc)


def attend(n_sp, layer, h, g_q, wq, k_all, v_all):
    tokens, depth = h.shape
    _, heads, _, head_dim = wq.shape
    bf, f32 = jnp.bfloat16, jnp.float32
    dma = pltpu.SemaphoreType.DMA
    bufs = 3
    any_spec = pl.BlockSpec(memory_space=pl.ANY)
    vmem = pl.BlockSpec(memory_space=pltpu.VMEM)
    return pl.pallas_call(
        functools.partial(attend_kernel, n_sp, layer),
        out_shape=jax.ShapeDtypeStruct((tokens, heads * head_dim), bf),
        in_specs=[vmem, vmem, any_spec, any_spec, any_spec],
        out_specs=vmem,
        scratch_shapes=[
            pltpu.VMEM((3, GROUP, depth, head_dim), bf),
            pltpu.VMEM((tokens, depth), bf),
            pltpu.VMEM((bufs, 2, heads, tokens, head_dim), bf),
            pltpu.VMEM((bufs, 2, heads, head_dim, tokens), bf),
            pltpu.VMEM((heads, head_dim, tokens), bf),
            pltpu.VMEM((heads, 8, tokens), f32),
            pltpu.VMEM((heads, 8, tokens), f32),
            pltpu.VMEM((heads, head_dim // 8, 8, tokens), f32),
            pltpu.VMEM((tokens // 4, 8, tokens), f32),
            pltpu.VMEM((tokens // 4, 8, tokens), f32),
            dma((3,)),
            dma((bufs, 2)),
        ],
        compiler_params=pltpu.CompilerParams(vmem_limit_bytes=VMEM_LIMIT),
        name="attend",
    )(h, g_q, wq, k_all, v_all)


def tail_kernel(
    layer, o_ref, h_ref, g_ref, wo_hbm, wg_hbm, wu_hbm, wd_hbm, out_ref,
    wo, wg, wu, wd, hm, nb, acc, mb, o_sem, w_sem,
):
    tokens, depth = h_ref.shape
    parts, _, o_cols = wo.shape
    bufs, _, cols = wg.shape
    steps = wg_hbm.shape[2] // cols
    sub = math.gcd(cols, 256)
    span = math.gcd(depth, 512)

    def o_copy(j):
        return pltpu.make_async_copy(
            wo_hbm.at[layer, :, pl.ds(j * o_cols, o_cols)], wo.at[j], o_sem.at[j])

    def w_copies(i, slot):
        sl = pl.ds(pl.multiple_of(i * cols, cols), cols)
        return (
            pltpu.make_async_copy(wg_hbm.at[layer, :, sl], wg.at[slot], w_sem.at[slot, 0]),
            pltpu.make_async_copy(wu_hbm.at[layer, :, sl], wu.at[slot], w_sem.at[slot, 1]),
            pltpu.make_async_copy(wd_hbm.at[layer, sl, :], wd.at[slot], w_sem.at[slot, 2]),
        )

    queue = [[o_copy(j)] for j in range(parts)]
    for i in range(min(bufs - 1, steps)):
        queue += [[copy] for copy in w_copies(i, i)]
    for item in queue[:3]:
        item[0].start()
    queue = queue[3:]

    for j in range(parts):
        o_copy(j).wait()
        for item in queue[:2]:
            item[0].start()
        queue = queue[2:]
        sl = slice(j * o_cols, (j + 1) * o_cols)
        r = jnp.dot(o_ref[...], wo[j], preferred_element_type=jnp.float32)
        h = (h_ref[:, sl].astype(jnp.float32) + r).astype(jnp.bfloat16)
        hm[:, sl] = h
        acc[:, sl] = h.astype(jnp.float32)
    for item in queue:
        item[0].start()
    norm_rows(hm, g_ref[layer:layer + 1, :], nb)

    @pl.loop(0, steps)
    def _(i):
        slot = lax.rem(i, bufs)
        for copy in w_copies(i, slot):
            copy.wait()

        @pl.when(i + bufs - 1 < steps)
        def _():
            for copy in w_copies(i + bufs - 1, lax.rem(i + bufs - 1, bufs)):
                copy.start()

        n = nb[...]
        for s in range(cols // sub):
            sl = slice(s * sub, (s + 1) * sub)
            a = jnp.dot(n, wg[slot, :, sl], preferred_element_type=jnp.float32)
            b = jnp.dot(n, wu[slot, :, sl], preferred_element_type=jnp.float32)
            mb[:, sl] = (jax.nn.silu(a) * b).astype(jnp.bfloat16)
        m = mb[...]
        for t in range(depth // span):
            sl = slice(t * span, (t + 1) * span)
            acc[:, sl] += jnp.dot(m, wd[slot, :, sl], preferred_element_type=jnp.float32)

    out_ref[...] = acc[...].astype(jnp.bfloat16)


def tail(layer, o, h, g, wo, wg, wu, wd):
    tokens, depth = h.shape
    ff = wg.shape[2]
    bf, f32 = jnp.bfloat16, jnp.float32
    dma = pltpu.SemaphoreType.DMA
    bufs = 3
    cols = math.gcd(ff, 768)
    o_cols = math.gcd(depth, 512)
    parts = depth // o_cols
    any_spec = pl.BlockSpec(memory_space=pl.ANY)
    vmem = pl.BlockSpec(memory_space=pltpu.VMEM)
    return pl.pallas_call(
        functools.partial(tail_kernel, layer),
        out_shape=jax.ShapeDtypeStruct((tokens, depth), bf),
        in_specs=[vmem, vmem, vmem] + [any_spec] * 4,
        out_specs=vmem,
        scratch_shapes=[
            pltpu.VMEM((parts, wo.shape[1], o_cols), bf),
            pltpu.VMEM((bufs, depth, cols), bf),
            pltpu.VMEM((bufs, depth, cols), bf),
            pltpu.VMEM((bufs, cols, depth), bf),
            pltpu.VMEM((tokens, depth), bf),
            pltpu.VMEM((tokens, depth), bf),
            pltpu.VMEM((tokens, depth), f32),
            pltpu.VMEM((tokens, cols), bf),
            dma((parts,)),
            dma((bufs, 3)),
        ],
        compiler_params=pltpu.CompilerParams(vmem_limit_bytes=VMEM_LIMIT),
        name="tail",
    )(o, h, g, wo, wg, wu, wd)


def solution(mesh):
    n_sp = mesh.shape["sp"]
    row_spec = P(("dp", "sp"), None)
    in_specs = (row_spec,) + (P(),) * 10

    def local_block(x, g_kv, w_k, w_v, g_attn, w_q, w_o, g_mlp, w_gate, w_up, w_down):
        depth = x.shape[1]
        wk = w_k.transpose(1, 0, 2)
        wv = w_v.transpose(1, 0, 2)
        wq = w_q.transpose(0, 2, 1, 3)
        wo = w_o.reshape(w_o.shape[0], -1, depth)
        k_all, v_all, o = gather_attend(
            n_sp, x, g_kv, g_attn, wk, wv, wq)
        h = tail(0, o, x, g_mlp, wo, w_gate, w_up, w_down)
        for layer in range(1, w_q.shape[0]):
            o = attend(n_sp, layer, h, g_attn, wq, k_all, v_all)
            h = tail(layer, o, h, g_mlp, wo, w_gate, w_up, w_down)
        return h

    return jax.shard_map(local_block, mesh=mesh, in_specs=in_specs, out_specs=row_spec, check_vma=False)
```

```python
import functools
import math

import jax
import jax.numpy as jnp
from jax import lax
from jax.experimental import pallas as pl
from jax.experimental.pallas import tpu as pltpu
from jax.sharding import PartitionSpec as P

EPS = 1e-6
LOG2E = 1.4426950408889634
MESH = pl.DeviceIdType.MESH
VMEM_LIMIT = 67043328
GROUP = 4


def norm_rows(src, gain, dst):
    rows = src.shape[0]
    step = math.gcd(rows, 16)
    g = gain.astype(jnp.float32)

    def body(i, carry):
        sl = pl.ds(pl.multiple_of(i * step, step), step)
        v = src[sl, :].astype(jnp.float32)
        inv = lax.rsqrt(jnp.mean(v * v, axis=-1, keepdims=True) + EPS)
        dst[sl, :] = (v * inv * g).astype(jnp.bfloat16)
        return carry

    lax.fori_loop(0, rows // step, body, 0, unroll=4)


def heads_matrix(w):
    return jnp.concatenate([w[i] for i in range(GROUP)], axis=1)


def project(n, w):
    return jnp.dot(n, heads_matrix(w), preferred_element_type=jnp.float32).astype(jnp.bfloat16)


def all_sublanes(x, op):
    for shift in (4, 2, 1):
        x = op(x, pltpu.roll(x, shift, 0))
    return x


def attend_block(ks, vs, q_ref, m_ref, l_ref, acc_ref, s_refs, masks=None, unroll=4):
    heads, size, head_dim = ks[0].shape
    tokens = q_ref.shape[2]
    scale = LOG2E * head_dim ** -0.5
    n = size // 8

    def scores(h, s_ref):
        top = None
        for i, k in enumerate(ks):
            s = jnp.dot(k[h], q_ref[h], preferred_element_type=jnp.float32)
            if masks is not None:
                s = jnp.where(masks[i], s, -jnp.inf)
            s = s.reshape(n, 8, tokens)
            s_ref[i * n:(i + 1) * n] = s
            t = jnp.max(s, axis=0)
            top = t if top is None else jnp.maximum(top, t)
        return all_sublanes(top, jnp.maximum)

    def update(h, s_ref, top):
        m_old = m_ref[h]
        m_new = jnp.maximum(m_old, top * scale)
        alpha = jnp.exp2(m_old - m_new)
        m_ref[h] = m_new
        p = jnp.exp2(s_ref[:n * len(ks)] * scale - m_new[None])
        l_ref[h] = l_ref[h] * alpha + jnp.sum(p, axis=0)
        p = p.reshape(size * len(ks), tokens).astype(jnp.bfloat16)
        v = jnp.concatenate([r[h] for r in vs], axis=1) if len(vs) > 1 else vs[0][h]
        o = jnp.dot(v, p, preferred_element_type=jnp.float32)
        acc_ref[h] = acc_ref[h] * alpha[None] + o.reshape(head_dim // 8, 8, tokens)

    unroll = math.gcd(heads, unroll)

    def body(g, top):
        h = unroll * g
        for i in range(unroll):
            nxt = h + i + 1
            if i == unroll - 1:
                nxt = jnp.minimum(nxt, heads - 1)
            after = scores(nxt, s_refs[(i + 1) % 2])
            update(h + i, s_refs[i % 2], top)
            top = after
        return top

    lax.fori_loop(0, heads // unroll, body, scores(0, s_refs[0]))


def reset_state(m_ref, l_ref, acc_ref):
    m_ref[...] = jnp.full_like(m_ref, -jnp.inf)
    l_ref[...] = jnp.zeros_like(l_ref)

    @pl.loop(0, acc_ref.shape[0])
    def _(h):
        acc_ref[h] = jnp.zeros(acc_ref.shape[1:], jnp.float32)


def write_attention(o_ref, l_ref, acc_ref):
    heads, _, _, tokens = acc_ref.shape
    head_dim = o_ref.shape[1] // heads

    @pl.loop(0, heads)
    def _(h):
        inv = 1.0 / all_sublanes(l_ref[h], jnp.add)
        o = (acc_ref[h] * inv[None]).reshape(head_dim, tokens)
        cols = pl.ds(pl.multiple_of(h * head_dim, head_dim), head_dim)
        o_ref[:, cols] = o.astype(jnp.bfloat16).T


def causal_mask(tokens, half, core, d):
    shape = (2 * half, tokens)
    k = lax.broadcasted_iota(jnp.int32, shape, 0)
    q = lax.broadcasted_iota(jnp.int32, shape, 1)
    key_pos = jnp.where(k >= half, k - half + tokens, k) + d * half
    return key_pos <= q + core * tokens


def attend_valid(u, chip, chips, ks, vs, state):
    s = (u + 1) // 2

    @pl.when(chip + s >= chips)
    def _():
        attend_block(ks, vs, *state, unroll=10)

    @pl.when(jnp.logical_and(chip >= s, chip + s < chips))
    def _():
        attend_block(ks[:1], vs[:1], *state)


def gather_attend_kernel(
    n_sp, x_hbm, g_kv, g_q, wk_hbm, wv_hbm, wq_hbm,
    k_all, v_all, o_ref,
    wk, wv, wq, xs, nb, kb, vb, ka, va, qt, m_ref, l_ref, acc, s0, s1,
    x_sem, w_sem, q_sem, send_sem, recv_sem, st_sem, px_sem, pr_sem, ld_sem,
):
    heads, depth, head_dim = wk.shape
    tokens = nb.shape[0]
    half = tokens // 2
    groups = heads // GROUP
    chips = n_sp // 2
    me = lax.axis_index("sp")
    chip = me // 2
    core = me - 2 * chip
    right = lax.rem(me + 2, n_sp)
    left = lax.rem(me + n_sp - 2, n_sp)
    partner = me + 1 - 2 * core

    barrier = pltpu.get_barrier_semaphore()
    for dev in (left, right, partner):
        pl.semaphore_signal(barrier, inc=1, device_id={"sp": dev}, device_id_type=MESH)
    pl.semaphore_wait(barrier, 3)

    def hop(src, u, d):
        return pltpu.make_async_remote_copy(
            src_ref=src,
            dst_ref=xs.at[u, pl.ds(d * half, half), :],
            send_sem=send_sem.at[u, d],
            recv_sem=recv_sem.at[u, d],
            device_id={"sp": right if d == 0 else left},
            device_id_type=MESH,
        )

    def own(u, d):
        return hop(x_hbm.at[pl.ds((u - 1) * half, half), :], u, d)

    def relay(u_from, u, d):
        return hop(xs.at[u_from, pl.ds(d * half, half), :], u, d)

    for u in (1, 2):
        for d in (0, 1):
            own(u, d).start()
    x_copy = pltpu.make_async_copy(x_hbm, xs.at[0], x_sem)
    x_copy.start()

    def w_copy(which, j):
        src, dst = ((wk_hbm, wk), (wv_hbm, wv))[which]
        sl = pl.ds(j * GROUP, GROUP)
        return pltpu.make_async_copy(src.at[sl], dst.at[sl], w_sem.at[which, j])

    def q_copy(j, slot):
        return pltpu.make_async_copy(
            wq_hbm.at[0, pl.ds(j * GROUP, GROUP)], wq.at[slot], q_sem.at[slot])

    ahead = min(2, groups)
    for j in range(ahead):
        w_copy(0, j).start()
        w_copy(1, j).start()
    reset_state(m_ref, l_ref, acc)
    x_copy.wait()

    cuts = [0, (groups + 1) // 2 * GROUP, heads]

    def stores(u, slot, j):
        out = []
        hs = pl.ds(cuts[j], cuts[j + 1] - cuts[j])
        for i, (buf, full) in enumerate(((kb, k_all), (vb, v_all))):
            for d in (0, 1):
                part = pl.ds(d * half, half)
                mine = pl.ds(core * half, half)
                if i == 0:
                    src, dst = buf.at[slot, hs, part, :], full.at[u, d, hs, mine, :]
                else:
                    src, dst = buf.at[slot, hs, :, part], full.at[u, d, hs, :, mine]
                local = pltpu.make_async_copy(src, dst, st_sem.at[slot, j, i, d])
                remote = pltpu.make_async_remote_copy(
                    src_ref=src, dst_ref=dst,
                    send_sem=px_sem.at[slot, j, i, d], recv_sem=pr_sem.at[u, j, i, d],
                    device_id={"sp": partner}, device_id_type=MESH,
                )
                out.append((local, remote))
        return out

    def loads(u):
        out = []
        for d in (0, 1):
            out.append(pltpu.make_async_copy(k_all.at[u, d], ka.at[d], ld_sem.at[d, 0]))
            out.append(pltpu.make_async_copy(v_all.at[u, d], va.at[d], ld_sem.at[d, 1]))
        return out

    def finish_stores(u):
        for j in (0, 1):
            for local, remote in stores(u, lax.rem(u, 2), j):
                local.wait()
                remote.wait_send()
                remote.wait_recv()

    state = (qt, m_ref, l_ref, acc, (s0, s1))

    def attend_unit(u):
        for copy in loads(u):
            copy.wait()
        attend_valid(u, chip, chips, [ka.at[0], ka.at[1]], [va.at[0], va.at[1]], state)

    def attend_own():
        for copy in loads(0):
            copy.wait()
        masks = [causal_mask(tokens, half, core, d) for d in (0, 1)]
        attend_block([ka.at[0], ka.at[1]], [va.at[0], va.at[1]], *state, masks=masks)

    def start_stores(u, slot, j):
        for local, remote in stores(u, slot, j):
            local.start()
            remote.start()

    def make_kv(slot, j):
        sl = pl.ds(j * GROUP, GROUP)
        n = nb[...]
        k = project(n, wk[sl])
        v = project(n, wv[sl])
        for i in range(GROUP):
            cols = slice(i * head_dim, (i + 1) * head_dim)
            kb[slot, j * GROUP + i] = k[:, cols]
            vb[slot, j * GROUP + i] = v[:, cols].T

    norm_rows(xs.at[0], g_kv[...].reshape(1, depth), nb)

    @pl.loop(0, groups)
    def _(j):
        w_copy(0, j).wait()
        w_copy(1, j).wait()

        @pl.when(j + ahead < groups)
        def _():
            w_copy(0, j + ahead).start()
            w_copy(1, j + ahead).start()

        @pl.when(j + ahead >= groups)
        def _():
            q_copy(j + ahead - groups, j + ahead - groups).start()

        make_kv(0, j)

    for j in (0, 1):
        start_stores(0, 0, j)
    norm_rows(xs.at[0], g_q[0:1, :], nb)

    @pl.loop(0, groups)
    def _(j):
        qslot = lax.rem(j, 2)
        q_copy(j, qslot).wait()
        q = project(nb[...], wq[qslot])
        for i in range(GROUP):
            qt[j * GROUP + i] = q[:, i * head_dim:(i + 1) * head_dim].T

        @pl.when(j + 2 < groups)
        def _():
            q_copy(j + 2, qslot).start()

    @pl.loop(1, chips + 1)
    def _(u):
        @pl.when(u < chips)
        def _():
            for d in (0, 1):
                relay(0, u, d).wait_recv()

        @pl.when(u <= chips - 4)
        def _():
            for d in (0, 1):
                relay(u, u + 2, d).start()

        @pl.when(u == chips - 3)
        def _():
            relay(u, u + 2, 0).start()

        @pl.when(u == chips - 2)
        def _():
            relay(u, u + 1, 1).start()

        finish_stores(u - 1)
        for copy in loads(u - 1):
            copy.start()

        @pl.when(u < chips)
        def _():
            norm_rows(xs.at[u], g_kv[...].reshape(1, depth), nb)
            for j in range(groups):
                make_kv(lax.rem(u, 2), j)
                for i in (0, 1):
                    if (j + 1) * GROUP == cuts[i + 1]:
                        start_stores(u, lax.rem(u, 2), i)

        @pl.when(u == 1)
        def _():
            attend_own()

        @pl.when(u >= 2)
        def _():
            attend_unit(u - 1)

    write_attention(o_ref, l_ref, acc)
    for u in range(1, chips):
        for d in (0, 1):
            relay(0, u, d).wait_send()


def gather_attend(n_sp, x, g_kv, g_q, wk, wv, wq):
    tokens, depth = x.shape
    heads, _, head_dim = wk.shape
    chips = n_sp // 2
    bf, f32 = jnp.bfloat16, jnp.float32
    dma = pltpu.SemaphoreType.DMA
    groups = heads // GROUP
    any_spec = pl.BlockSpec(memory_space=pl.ANY)
    vmem = pl.BlockSpec(memory_space=pltpu.VMEM)
    return pl.pallas_call(
        functools.partial(gather_attend_kernel, n_sp),
        out_shape=(
            jax.ShapeDtypeStruct((chips, 2, heads, tokens, head_dim), bf),
            jax.ShapeDtypeStruct((chips, 2, heads, head_dim, tokens), bf),
            jax.ShapeDtypeStruct((tokens, heads * head_dim), bf),
        ),
        in_specs=[any_spec, vmem, vmem, any_spec, any_spec, any_spec],
        out_specs=(any_spec, any_spec, vmem),
        scratch_shapes=[
            pltpu.VMEM((heads, depth, head_dim), bf),
            pltpu.VMEM((heads, depth, head_dim), bf),
            pltpu.VMEM((2, GROUP, depth, head_dim), bf),
            pltpu.VMEM((chips, tokens, depth), bf),
            pltpu.VMEM((tokens, depth), bf),
            pltpu.VMEM((2, heads, tokens, head_dim), bf),
            pltpu.VMEM((2, heads, head_dim, tokens), bf),
            pltpu.VMEM((2, heads, tokens, head_dim), bf),
            pltpu.VMEM((2, heads, head_dim, tokens), bf),
            pltpu.VMEM((heads, head_dim, tokens), bf),
            pltpu.VMEM((heads, 8, tokens), f32),
            pltpu.VMEM((heads, 8, tokens), f32),
            pltpu.VMEM((heads, head_dim // 8, 8, tokens), f32),
            pltpu.VMEM((tokens // 4, 8, tokens), f32),
            pltpu.VMEM((tokens // 4, 8, tokens), f32),
            dma,
            dma((2, groups)),
            dma((2,)),
            dma((chips, 2)),
            dma((chips, 2)),
            dma((2, 2, 2, 2)),
            dma((2, 2, 2, 2)),
            dma((chips, 2, 2, 2)),
            dma((2, 2)),
        ],
        compiler_params=pltpu.CompilerParams(
            collective_id=0, has_side_effects=True, vmem_limit_bytes=VMEM_LIMIT
        ),
        name="gather_attend",
    )(x, g_kv, g_q, wk, wv, wq)


def rest_kernel(
    n_sp, o_hbm, x_hbm, g_attn, g_mlp, wq_hbm, wo_hbm, wg_hbm, wu_hbm, wd_hbm, k_all, v_all,
    h_ref,
    wb, wg, wu, wd, ka, va, qt, m_ref, l_ref, acc, s0, s1, ob, nb, sums, mb,
    b_sem, w_sem, ld_sem, in_sem,
):
    layers, heads, depth, head_dim = wq_hbm.shape
    tokens = nb.shape[0]
    half = tokens // 2
    groups = heads // GROUP
    chips = n_sp // 2
    blocks = depth // head_dim
    cols = wg.shape[2]
    steps = wg_hbm.shape[2] // cols
    sub = math.gcd(cols, 256)
    span = math.gcd(depth, 512)
    me = lax.axis_index("sp")
    chip = me // 2
    core = me - 2 * chip

    def q_copy(layer, j):
        return pltpu.make_async_copy(wq_hbm.at[layer, j], wb.at[j], b_sem.at[j])

    def o_copy(layer, j):
        return pltpu.make_async_copy(
            wo_hbm.at[layer, :, pl.ds(j * head_dim, head_dim)], wb.at[j], b_sem.at[j])

    def w_copies(layer, i, slot):
        sl = pl.ds(pl.multiple_of(i * cols, cols), cols)
        return (
            pltpu.make_async_copy(wg_hbm.at[layer, :, sl], wg.at[slot], w_sem.at[slot, 0]),
            pltpu.make_async_copy(wu_hbm.at[layer, :, sl], wu.at[slot], w_sem.at[slot, 1]),
            pltpu.make_async_copy(wd_hbm.at[layer, sl, :], wd.at[slot], w_sem.at[slot, 2]),
        )

    def loads(u, slot):
        return (
            pltpu.make_async_copy(k_all.at[u], ka.at[slot], ld_sem.at[slot, 0]),
            pltpu.make_async_copy(v_all.at[u], va.at[slot], ld_sem.at[slot, 1]),
        )

    def output_projection(layer, queue):
        for j in range(blocks // GROUP):
            for i in range(GROUP):
                o_copy(layer, j * GROUP + i).wait()
            for copy in queue[j * GROUP:(j + 1) * GROUP]:
                copy.start()
            sl = slice(j * GROUP * head_dim, (j + 1) * GROUP * head_dim)
            w = heads_matrix(wb[j * GROUP:(j + 1) * GROUP])
            r = jnp.dot(ob[...], w, preferred_element_type=jnp.float32)
            h = (h_ref[:, sl].astype(jnp.float32) + r).astype(jnp.bfloat16)
            h_ref[:, sl] = h
            sums[:, sl] = h.astype(jnp.float32)

    def mlp(layer):
        norm_rows(h_ref, g_mlp[layer:layer + 1, :], nb)

        @pl.loop(0, steps)
        def _(i):
            slot = lax.rem(i, 2)
            for copy in w_copies(layer, i, slot):
                copy.wait()
            n = nb[...]
            for s in range(cols // sub):
                sl = slice(s * sub, (s + 1) * sub)
                a = jnp.dot(n, wg[slot, :, sl], preferred_element_type=jnp.float32)
                b = jnp.dot(n, wu[slot, :, sl], preferred_element_type=jnp.float32)
                mb[:, sl] = (jax.nn.silu(a) * b).astype(jnp.bfloat16)

            @pl.when(i + 2 < steps)
            def _():
                for copy in w_copies(layer, i + 2, slot)[:2]:
                    copy.start()

            if layer + 1 < layers:
                @pl.when(i == steps - 2)
                def _():
                    for j in range(heads):
                        q_copy(layer + 1, j).start()

                @pl.when(i == steps - 1)
                def _():
                    for u in (0, 1):
                        for copy in loads(u, u):
                            copy.start()

            m = mb[...]
            for t in range(depth // span):
                sl = slice(t * span, (t + 1) * span)
                sums[:, sl] += jnp.dot(m, wd[slot, :, sl], preferred_element_type=jnp.float32)

            @pl.when(i + 2 < steps)
            def _():
                w_copies(layer, i + 2, slot)[2].start()

        h_ref[...] = sums[...].astype(jnp.bfloat16)

    def attention(layer):
        norm_rows(h_ref, g_attn[layer:layer + 1, :], nb)
        reset_state(m_ref, l_ref, acc)
        for j in range(heads):
            q_copy(layer, j).wait()
        for j in range(groups):
            q = project(nb[...], wb[j * GROUP:(j + 1) * GROUP])
            for i in range(GROUP):
                qt[j * GROUP + i] = q[:, i * head_dim:(i + 1) * head_dim].T

        state = (qt, m_ref, l_ref, acc, (s0, s1))
        first = w_copies(layer, 0, 0)
        second = w_copies(layer, 1, 1)
        ahead = [[o_copy(layer, j) for j in range(blocks)], [], first[:2], first[2:],
                 second[:1], second[1:2], second[2:]]

        @pl.loop(0, chips)
        def _(u):
            slot = lax.rem(u, 2)
            for copy in loads(u, slot):
                copy.wait()
            for i, copies in enumerate(ahead):
                if copies:
                    @pl.when(u == i)
                    def _(copies=copies):
                        for copy in copies:
                            copy.start()

            ks = [ka.at[slot, d] for d in (0, 1)]
            vs = [va.at[slot, d] for d in (0, 1)]

            @pl.when(u == 0)
            def _():
                masks = [causal_mask(tokens, half, core, d) for d in (0, 1)]
                attend_block(ks, vs, *state, masks=masks)

            @pl.when(u > 0)
            def _():
                attend_valid(u, chip, chips, ks, vs, state)

            @pl.when(u + 2 < chips)
            def _():
                for copy in loads(u + 2, slot):
                    copy.start()

        write_attention(ob, l_ref, acc)

    inputs = (pltpu.make_async_copy(o_hbm, ob, in_sem.at[0]),
              pltpu.make_async_copy(x_hbm, h_ref, in_sem.at[1]))
    for copy in inputs:
        copy.start()
    queue = [o_copy(0, j) for j in range(blocks)]
    for copy in queue[:2 * GROUP]:
        copy.start()
    first = w_copies(0, 0, 0)
    second = w_copies(0, 1, 1)
    queue = queue[2 * GROUP:]
    queue += [*first, *second]
    for copy in inputs:
        copy.wait()
    output_projection(0, queue)
    for copy in queue[blocks:]:
        copy.start()
    mlp(0)
    for layer in range(1, layers):
        attention(layer)
        output_projection(layer, [])
        mlp(layer)


def rest(n_sp, o, x, g_attn, g_mlp, wq, wo, wg, wu, wd, k_all, v_all):
    tokens, depth = x.shape
    _, heads, _, head_dim = wq.shape
    bf, f32 = jnp.bfloat16, jnp.float32
    dma = pltpu.SemaphoreType.DMA
    cols = math.gcd(wg.shape[2], 768)
    any_spec = pl.BlockSpec(memory_space=pl.ANY)
    vmem = pl.BlockSpec(memory_space=pltpu.VMEM)
    return pl.pallas_call(
        functools.partial(rest_kernel, n_sp),
        out_shape=jax.ShapeDtypeStruct((tokens, depth), bf),
        in_specs=[any_spec, any_spec, vmem, vmem] + [any_spec] * 7,
        out_specs=vmem,
        scratch_shapes=[
            pltpu.VMEM((max(heads, depth // head_dim), depth, head_dim), bf),
            pltpu.VMEM((2, depth, cols), bf),
            pltpu.VMEM((2, depth, cols), bf),
            pltpu.VMEM((2, cols, depth), bf),
            pltpu.VMEM((2, 2, heads, tokens, head_dim), bf),
            pltpu.VMEM((2, 2, heads, head_dim, tokens), bf),
            pltpu.VMEM((heads, head_dim, tokens), bf),
            pltpu.VMEM((heads, 8, tokens), f32),
            pltpu.VMEM((heads, 8, tokens), f32),
            pltpu.VMEM((heads, head_dim // 8, 8, tokens), f32),
            pltpu.VMEM((tokens // 4, 8, tokens), f32),
            pltpu.VMEM((tokens // 4, 8, tokens), f32),
            pltpu.VMEM((tokens, heads * head_dim), bf),
            pltpu.VMEM((tokens, depth), bf),
            pltpu.VMEM((tokens, depth), f32),
            pltpu.VMEM((tokens, cols), bf),
            dma((max(heads, depth // head_dim),)),
            dma((2, 3)),
            dma((2, 2)),
            dma((2,)),
        ],
        compiler_params=pltpu.CompilerParams(vmem_limit_bytes=VMEM_LIMIT),
        name="rest",
    )(o, x, g_attn, g_mlp, wq, wo, wg, wu, wd, k_all, v_all)


def solution(mesh):
    n_sp = mesh.shape["sp"]
    row_spec = P(("dp", "sp"), None)
    in_specs = (row_spec,) + (P(),) * 10

    def local_block(x, g_kv, w_k, w_v, g_attn, w_q, w_o, g_mlp, w_gate, w_up, w_down):
        depth = x.shape[1]
        wk = w_k.transpose(1, 0, 2)
        wv = w_v.transpose(1, 0, 2)
        wq = w_q.transpose(0, 2, 1, 3)
        wo = w_o.reshape(w_o.shape[0], -1, depth)
        k_all, v_all, o = gather_attend(
            n_sp, x, g_kv, g_attn, wk, wv, wq)
        h = rest(n_sp, o, x, g_attn, g_mlp, wq, wo, w_gate, w_up, w_down, k_all, v_all)
        return h

    return jax.shard_map(local_block, mesh=mesh, in_specs=in_specs, out_specs=row_spec, check_vma=False)
```

```python
import functools
import math

import jax
import jax.numpy as jnp
from jax import lax
from jax.experimental import pallas as pl
from jax.experimental.pallas import tpu as pltpu
from jax.sharding import PartitionSpec as P

EPS = 1e-6
LOG2E = 1.4426950408889634
MESH = pl.DeviceIdType.MESH
VMEM_LIMIT = 67043328
GROUP = 4


SLOTS = 5


def norm_rows(src, gain, dst):
    rows = src.shape[0]
    step = math.gcd(rows, 16)
    g = gain.astype(jnp.float32)

    def body(i, carry):
        sl = pl.ds(pl.multiple_of(i * step, step), step)
        v = src[sl, :].astype(jnp.float32)
        inv = lax.rsqrt(jnp.mean(v * v, axis=-1, keepdims=True) + EPS)
        dst[sl, :] = (v * inv * g).astype(jnp.bfloat16)
        return carry

    lax.fori_loop(0, rows // step, body, 0, unroll=4)


def heads_matrix(w):
    return jnp.concatenate([w[i] for i in range(GROUP)], axis=1)


def project(n, w):
    return jnp.dot(n, heads_matrix(w), preferred_element_type=jnp.float32).astype(jnp.bfloat16)


def all_sublanes(x, op):
    for shift in (4, 2, 1):
        x = op(x, pltpu.roll(x, shift, 0))
    return x


def attend_block(ks, vs, q_ref, m_ref, l_ref, acc_ref, s_refs, masks=None, unroll=10):
    heads, size, head_dim = ks[0].shape
    tokens = q_ref.shape[2]
    scale = LOG2E * head_dim ** -0.5
    n = size // 8

    def scores(h, s_ref):
        top = None
        for i, k in enumerate(ks):
            s = jnp.dot(k[h], q_ref[h], preferred_element_type=jnp.float32)
            if masks is not None:
                s = jnp.where(masks[i], s, -jnp.inf)
            s = s.reshape(n, 8, tokens)
            s_ref[i * n:(i + 1) * n] = s
            t = jnp.max(s, axis=0)
            top = t if top is None else jnp.maximum(top, t)
        return all_sublanes(top, jnp.maximum)

    def update(h, s_ref, top):
        m_old = m_ref[h]
        m_new = jnp.maximum(m_old, top * scale)
        alpha = jnp.exp2(m_old - m_new)
        m_ref[h] = m_new
        p = jnp.exp2(s_ref[:n * len(ks)] * scale - m_new[None])
        l_ref[h] = l_ref[h] * alpha + jnp.sum(p, axis=0)
        p = p.reshape(size * len(ks), tokens).astype(jnp.bfloat16)
        v = jnp.concatenate([r[h] for r in vs], axis=1) if len(vs) > 1 else vs[0][h]
        o = jnp.dot(v, p, preferred_element_type=jnp.float32)
        acc_ref[h] = acc_ref[h] * alpha[None] + o.reshape(head_dim // 8, 8, tokens)

    unroll = math.gcd(heads, unroll)
    assert unroll % len(s_refs) == 0

    depth = min(2, len(s_refs) - 1)

    def body(g, tops):
        h = unroll * g
        tops = list(tops)
        for i in range(unroll):
            nxt = h + i + depth
            if i >= unroll - depth:
                nxt = jnp.minimum(nxt, heads - 1)
            tops.append(scores(nxt, s_refs[(i + depth) % len(s_refs)]))
            update(h + i, s_refs[i % len(s_refs)], tops.pop(0))
        return tuple(tops)

    tops = tuple(scores(i, s_refs[i]) for i in range(depth))
    lax.fori_loop(0, heads // unroll, body, tops)


def reset_state(m_ref, l_ref, acc_ref):
    m_ref[...] = jnp.full_like(m_ref, -jnp.inf)
    l_ref[...] = jnp.zeros_like(l_ref)

    @pl.loop(0, acc_ref.shape[0])
    def _(h):
        acc_ref[h] = jnp.zeros(acc_ref.shape[1:], jnp.float32)


def write_attention(o_ref, l_ref, acc_ref):
    heads, _, _, tokens = acc_ref.shape
    head_dim = o_ref.shape[1] // heads

    def body(h, carry):
        inv = 1.0 / all_sublanes(l_ref[h], jnp.add)
        o = (acc_ref[h] * inv[None]).reshape(head_dim, tokens)
        cols = pl.ds(pl.multiple_of(h * head_dim, head_dim), head_dim)
        o_ref[:, cols] = o.astype(jnp.bfloat16).T
        return carry

    lax.fori_loop(0, heads, body, 0, unroll=4)


def causal_mask(tokens, half, core, d):
    shape = (2 * half, tokens)
    k = lax.broadcasted_iota(jnp.int32, shape, 0)
    q = lax.broadcasted_iota(jnp.int32, shape, 1)
    key_pos = jnp.where(k >= half, k - half + tokens, k) + d * half
    return key_pos <= q + core * tokens


def attend_valid(u, chip, chips, ks, vs, state):
    s = (u + 1) // 2

    @pl.when(chip + s >= chips)
    def _():
        attend_block(ks, vs, *state, unroll=10)

    @pl.when(jnp.logical_and(chip >= s, chip + s < chips))
    def _():
        attend_block(ks[:1], vs[:1], *state)


def gather_attend_kernel(
    n_sp, x_hbm, g_kv, g_q, wk_hbm, wv_hbm, wq_hbm,
    k_all, v_all, o_ref,
    wk, wv, wq, xs, nb, kb, vb, ka, va, qt, m_ref, l_ref, acc, s_refs,
    x_sem, w_sem, q_sem, send_sem, recv_sem, st_sem, px_sem, pr_sem, ld_sem,
):
    heads, depth, head_dim = wk.shape
    tokens = nb.shape[0]
    half = tokens // 2
    groups = heads // GROUP
    chips = n_sp // 2
    me = lax.axis_index("sp")
    chip = me // 2
    core = me - 2 * chip
    right = lax.rem(me + 2, n_sp)
    left = lax.rem(me + n_sp - 2, n_sp)
    partner = me + 1 - 2 * core

    barrier = pltpu.get_barrier_semaphore()
    for dev in (left, right, partner):
        pl.semaphore_signal(barrier, inc=1, device_id={"sp": dev}, device_id_type=MESH)
    pl.semaphore_wait(barrier, 3)

    def hop(src, u, d):
        return pltpu.make_async_remote_copy(
            src_ref=src,
            dst_ref=xs.at[u, pl.ds(d * half, half), :],
            send_sem=send_sem.at[u, d],
            recv_sem=recv_sem.at[u, d],
            device_id={"sp": right if d == 0 else left},
            device_id_type=MESH,
        )

    def own(u, d):
        return hop(x_hbm.at[pl.ds((u - 1) * half, half), :], u, d)

    def relay(u_from, u, d):
        return hop(xs.at[u_from, pl.ds(d * half, half), :], u, d)

    for u in (1, 2):
        for d in (0, 1):
            own(u, d).start()
    x_copy = pltpu.make_async_copy(x_hbm, xs.at[0], x_sem)
    x_copy.start()

    def w_copy(which, j):
        src, dst = ((wk_hbm, wk), (wv_hbm, wv))[which]
        sl = pl.ds(j * GROUP, GROUP)
        return pltpu.make_async_copy(src.at[sl], dst.at[sl], w_sem.at[which, j])

    def q_copy(j, slot):
        return pltpu.make_async_copy(
            wq_hbm.at[0, pl.ds(j * GROUP, GROUP)], wq.at[slot], q_sem.at[slot])

    ahead = min(2, groups)
    for j in range(ahead):
        w_copy(0, j).start()
        w_copy(1, j).start()
    reset_state(m_ref, l_ref, acc)
    x_copy.wait()

    cuts = [0, (groups + 1) // 2 * GROUP, heads]

    def stores(u, slot, j):
        out = []
        hs = pl.ds(cuts[j], cuts[j + 1] - cuts[j])
        for i, (buf, full) in enumerate(((kb, k_all), (vb, v_all))):
            for d in (0, 1):
                part = pl.ds(d * half, half)
                mine = pl.ds(core * half, half)
                if i == 0:
                    src, dst = buf.at[slot, hs, part, :], full.at[u, d, hs, mine, :]
                else:
                    src, dst = buf.at[slot, hs, :, part], full.at[u, d, hs, :, mine]
                local = pltpu.make_async_copy(src, dst, st_sem.at[slot, j, i, d])
                remote = pltpu.make_async_remote_copy(
                    src_ref=src, dst_ref=dst,
                    send_sem=px_sem.at[slot, j, i, d], recv_sem=pr_sem.at[u, j, i, d],
                    device_id={"sp": partner}, device_id_type=MESH,
                )
                out.append((local, remote))
        return out

    def loads(u, j):
        hs = pl.ds(cuts[j], cuts[j + 1] - cuts[j])
        out = []
        for d in (0, 1):
            out.append(pltpu.make_async_copy(k_all.at[u, d, hs], ka.at[d, hs], ld_sem.at[d, 0, j]))
            out.append(pltpu.make_async_copy(v_all.at[u, d, hs], va.at[d, hs], ld_sem.at[d, 1, j]))
        return out

    def finish_stores(u):
        for j in (0, 1):
            for local, remote in stores(u, lax.rem(u, 2), j):
                local.wait()
                remote.wait_send()
                remote.wait_recv()
            for copy in loads(u, j):
                copy.start()

    def wait_loads(u):
        for j in (0, 1):
            for copy in loads(u, j):
                copy.wait()

    state = (qt, m_ref, l_ref, acc, [s_refs.at[i] for i in range(s_refs.shape[0])])

    def attend_unit(u):
        wait_loads(u)
        attend_valid(u, chip, chips, [ka.at[0], ka.at[1]], [va.at[0], va.at[1]], state)

    def attend_own():
        wait_loads(0)
        masks = [causal_mask(tokens, half, core, d) for d in (0, 1)]
        attend_block([ka.at[0], ka.at[1]], [va.at[0], va.at[1]], *state, masks=masks)

    def start_stores(u, slot, j):
        for local, remote in stores(u, slot, j):
            local.start()
            remote.start()

    def make_kv(slot, j):
        sl = pl.ds(j * GROUP, GROUP)
        n = nb[...]
        k = project(n, wk[sl])
        v = project(n, wv[sl])
        for i in range(GROUP):
            cols = slice(i * head_dim, (i + 1) * head_dim)
            kb[slot, j * GROUP + i] = k[:, cols]
            vb[slot, j * GROUP + i] = v[:, cols].T

    norm_rows(xs.at[0], g_kv[...].reshape(1, depth), nb)

    @pl.loop(0, groups)
    def _(j):
        w_copy(0, j).wait()
        w_copy(1, j).wait()

        @pl.when(j + ahead < groups)
        def _():
            w_copy(0, j + ahead).start()
            w_copy(1, j + ahead).start()

        @pl.when(j + ahead >= groups)
        def _():
            q_copy(j + ahead - groups, j + ahead - groups).start()

        make_kv(0, j)

    for j in (0, 1):
        start_stores(0, 0, j)
    norm_rows(xs.at[0], g_q[0:1, :], nb)

    @pl.loop(0, groups)
    def _(j):
        qslot = lax.rem(j, 2)
        q_copy(j, qslot).wait()
        q = project(nb[...], wq[qslot])
        for i in range(GROUP):
            qt[j * GROUP + i] = q[:, i * head_dim:(i + 1) * head_dim].T

        @pl.when(j + 2 < groups)
        def _():
            q_copy(j + 2, qslot).start()

    @pl.loop(1, chips + 1)
    def _(u):
        @pl.when(u < chips)
        def _():
            for d in (0, 1):
                relay(0, u, d).wait_recv()

        @pl.when(u <= chips - 4)
        def _():
            for d in (0, 1):
                relay(u, u + 2, d).start()

        @pl.when(u == chips - 3)
        def _():
            relay(u, u + 2, 0).start()

        @pl.when(u == chips - 2)
        def _():
            relay(u, u + 1, 1).start()

        finish_stores(u - 1)

        @pl.when(u < chips)
        def _():
            norm_rows(xs.at[u], g_kv[...].reshape(1, depth), nb)
            for j in range(groups):
                make_kv(lax.rem(u, 2), j)
                for i in (0, 1):
                    if (j + 1) * GROUP == cuts[i + 1]:
                        start_stores(u, lax.rem(u, 2), i)

        @pl.when(u == 1)
        def _():
            attend_own()

        @pl.when(u >= 2)
        def _():
            attend_unit(u - 1)

    write_attention(o_ref, l_ref, acc)
    for u in range(1, chips):
        for d in (0, 1):
            relay(0, u, d).wait_send()


def gather_attend(n_sp, x, g_kv, g_q, wk, wv, wq):
    tokens, depth = x.shape
    heads, _, head_dim = wk.shape
    chips = n_sp // 2
    bf, f32 = jnp.bfloat16, jnp.float32
    dma = pltpu.SemaphoreType.DMA
    groups = heads // GROUP
    any_spec = pl.BlockSpec(memory_space=pl.ANY)
    vmem = pl.BlockSpec(memory_space=pltpu.VMEM)
    return pl.pallas_call(
        functools.partial(gather_attend_kernel, n_sp),
        out_shape=(
            jax.ShapeDtypeStruct((chips, 2, heads, tokens, head_dim), bf),
            jax.ShapeDtypeStruct((chips, 2, heads, head_dim, tokens), bf),
            jax.ShapeDtypeStruct((tokens, heads * head_dim), bf),
        ),
        in_specs=[any_spec, vmem, vmem, any_spec, any_spec, any_spec],
        out_specs=(any_spec, any_spec, vmem),
        scratch_shapes=[
            pltpu.VMEM((heads, depth, head_dim), bf),
            pltpu.VMEM((heads, depth, head_dim), bf),
            pltpu.VMEM((2, GROUP, depth, head_dim), bf),
            pltpu.VMEM((chips, tokens, depth), bf),
            pltpu.VMEM((tokens, depth), bf),
            pltpu.VMEM((2, heads, tokens, head_dim), bf),
            pltpu.VMEM((2, heads, head_dim, tokens), bf),
            pltpu.VMEM((2, heads, tokens, head_dim), bf),
            pltpu.VMEM((2, heads, head_dim, tokens), bf),
            pltpu.VMEM((heads, head_dim, tokens), bf),
            pltpu.VMEM((heads, 8, tokens), f32),
            pltpu.VMEM((heads, 8, tokens), f32),
            pltpu.VMEM((heads, head_dim // 8, 8, tokens), f32),
            pltpu.VMEM((SLOTS, tokens // 4, 8, tokens), f32),
            dma,
            dma((2, groups)),
            dma((2,)),
            dma((chips, 2)),
            dma((chips, 2)),
            dma((2, 2, 2, 2)),
            dma((2, 2, 2, 2)),
            dma((chips, 2, 2, 2)),
            dma((2, 2, 2)),
        ],
        compiler_params=pltpu.CompilerParams(
            collective_id=0, has_side_effects=True, vmem_limit_bytes=VMEM_LIMIT
        ),
        name="gather_attend",
    )(x, g_kv, g_q, wk, wv, wq)


def rest_kernel(
    n_sp, o_hbm, x_hbm, g_attn, g_mlp, wq_hbm, wo_hbm, wg_hbm, wu_hbm, wd_hbm, k_all, v_all,
    h_ref,
    wb, wg, wu, wd, ka, va, qt, m_ref, l_ref, acc, s_refs, ob, nb, sums, mb,
    b_sem, w_sem, ld_sem, in_sem,
):
    layers, heads, depth, head_dim = wq_hbm.shape
    tokens = nb.shape[0]
    half = tokens // 2
    groups = heads // GROUP
    chips = n_sp // 2
    blocks = depth // head_dim
    cols = wg.shape[2]
    steps = wg_hbm.shape[2] // cols
    sub = math.gcd(cols, 256)
    span = math.gcd(depth, 512)
    me = lax.axis_index("sp")
    chip = me // 2
    core = me - 2 * chip

    def q_copy(layer, j):
        return pltpu.make_async_copy(wq_hbm.at[layer, j], wb.at[j], b_sem.at[j])

    def o_copy(layer, j):
        return pltpu.make_async_copy(
            wo_hbm.at[layer, :, pl.ds(j * head_dim, head_dim)], wb.at[j], b_sem.at[j])

    def w_copies(layer, i, slot):
        sl = pl.ds(pl.multiple_of(i * cols, cols), cols)
        return (
            pltpu.make_async_copy(wg_hbm.at[layer, :, sl], wg.at[slot], w_sem.at[slot, 0]),
            pltpu.make_async_copy(wu_hbm.at[layer, :, sl], wu.at[slot], w_sem.at[slot, 1]),
            pltpu.make_async_copy(wd_hbm.at[layer, sl, :], wd.at[slot], w_sem.at[slot, 2]),
        )

    def loads(u, slot):
        return (
            pltpu.make_async_copy(k_all.at[u], ka.at[slot], ld_sem.at[slot, 0]),
            pltpu.make_async_copy(v_all.at[u], va.at[slot], ld_sem.at[slot, 1]),
        )

    def output_projection(layer, queue):
        for j in range(blocks // GROUP):
            for i in range(GROUP):
                o_copy(layer, j * GROUP + i).wait()
            for copy in queue[j * GROUP:(j + 1) * GROUP]:
                copy.start()
            sl = slice(j * GROUP * head_dim, (j + 1) * GROUP * head_dim)
            w = heads_matrix(wb[j * GROUP:(j + 1) * GROUP])
            r = jnp.dot(ob[...], w, preferred_element_type=jnp.float32)
            h = (h_ref[:, sl].astype(jnp.float32) + r).astype(jnp.bfloat16)
            h_ref[:, sl] = h
            sums[:, sl] = h.astype(jnp.float32)

    def mlp(layer):
        norm_rows(h_ref, g_mlp[layer:layer + 1, :], nb)

        @pl.loop(0, steps)
        def _(i):
            slot = lax.rem(i, 2)
            for copy in w_copies(layer, i, slot):
                copy.wait()
            n = nb[...]
            for s in range(cols // sub):
                sl = slice(s * sub, (s + 1) * sub)
                a = jnp.dot(n, wg[slot, :, sl], preferred_element_type=jnp.float32)
                b = jnp.dot(n, wu[slot, :, sl], preferred_element_type=jnp.float32)
                mb[:, sl] = (jax.nn.silu(a) * b).astype(jnp.bfloat16)

            @pl.when(i + 2 < steps)
            def _():
                for copy in w_copies(layer, i + 2, slot)[:2]:
                    copy.start()

            if layer + 1 < layers:
                @pl.when(i == steps - 2)
                def _():
                    for j in range(heads):
                        q_copy(layer + 1, j).start()

                @pl.when(i == steps - 1)
                def _():
                    for u in (0, 1):
                        for copy in loads(u, u):
                            copy.start()

            m = mb[...]
            for t in range(depth // span):
                sl = slice(t * span, (t + 1) * span)
                sums[:, sl] += jnp.dot(m, wd[slot, :, sl], preferred_element_type=jnp.float32)

            @pl.when(i + 2 < steps)
            def _():
                w_copies(layer, i + 2, slot)[2].start()

        h_ref[...] = sums[...].astype(jnp.bfloat16)

    def attention(layer):
        norm_rows(h_ref, g_attn[layer:layer + 1, :], nb)
        reset_state(m_ref, l_ref, acc)
        for j in range(heads):
            q_copy(layer, j).wait()
        for j in range(groups):
            q = project(nb[...], wb[j * GROUP:(j + 1) * GROUP])
            for i in range(GROUP):
                qt[j * GROUP + i] = q[:, i * head_dim:(i + 1) * head_dim].T

        state = (qt, m_ref, l_ref, acc, [s_refs.at[i] for i in range(s_refs.shape[0])])
        first = w_copies(layer, 0, 0)
        second = w_copies(layer, 1, 1)
        ahead = [[o_copy(layer, j) for j in range(blocks)], [], first[:2], first[2:],
                 second[:1], second[1:2], second[2:]]

        @pl.loop(0, chips)
        def _(u):
            slot = lax.rem(u, 2)
            for copy in loads(u, slot):
                copy.wait()
            for i, copies in enumerate(ahead):
                if copies:
                    @pl.when(u == i)
                    def _(copies=copies):
                        for copy in copies:
                            copy.start()

            ks = [ka.at[slot, d] for d in (0, 1)]
            vs = [va.at[slot, d] for d in (0, 1)]

            @pl.when(u == 0)
            def _():
                masks = [causal_mask(tokens, half, core, d) for d in (0, 1)]
                attend_block(ks, vs, *state, masks=masks)

            @pl.when(u > 0)
            def _():
                attend_valid(u, chip, chips, ks, vs, state)

            @pl.when(u + 2 < chips)
            def _():
                for copy in loads(u + 2, slot):
                    copy.start()

        write_attention(ob, l_ref, acc)

    inputs = (pltpu.make_async_copy(o_hbm, ob, in_sem.at[0]),
              pltpu.make_async_copy(x_hbm, h_ref, in_sem.at[1]))
    for copy in inputs:
        copy.start()
    queue = [o_copy(0, j) for j in range(blocks)]
    for copy in queue[:2 * GROUP]:
        copy.start()
    first = w_copies(0, 0, 0)
    second = w_copies(0, 1, 1)
    queue = queue[2 * GROUP:]
    queue += [*first, *second]
    for copy in inputs:
        copy.wait()
    output_projection(0, queue)
    for copy in queue[blocks:]:
        copy.start()
    mlp(0)
    for layer in range(1, layers):
        attention(layer)
        output_projection(layer, [])
        mlp(layer)


def rest(n_sp, o, x, g_attn, g_mlp, wq, wo, wg, wu, wd, k_all, v_all):
    tokens, depth = x.shape
    _, heads, _, head_dim = wq.shape
    bf, f32 = jnp.bfloat16, jnp.float32
    dma = pltpu.SemaphoreType.DMA
    cols = math.gcd(wg.shape[2], 768)
    any_spec = pl.BlockSpec(memory_space=pl.ANY)
    vmem = pl.BlockSpec(memory_space=pltpu.VMEM)
    return pl.pallas_call(
        functools.partial(rest_kernel, n_sp),
        out_shape=jax.ShapeDtypeStruct((tokens, depth), bf),
        in_specs=[any_spec, any_spec, vmem, vmem] + [any_spec] * 7,
        out_specs=vmem,
        scratch_shapes=[
            pltpu.VMEM((max(heads, depth // head_dim), depth, head_dim), bf),
            pltpu.VMEM((2, depth, cols), bf),
            pltpu.VMEM((2, depth, cols), bf),
            pltpu.VMEM((2, cols, depth), bf),
            pltpu.VMEM((2, 2, heads, tokens, head_dim), bf),
            pltpu.VMEM((2, 2, heads, head_dim, tokens), bf),
            pltpu.VMEM((heads, head_dim, tokens), bf),
            pltpu.VMEM((heads, 8, tokens), f32),
            pltpu.VMEM((heads, 8, tokens), f32),
            pltpu.VMEM((heads, head_dim // 8, 8, tokens), f32),
            pltpu.VMEM((SLOTS, tokens // 4, 8, tokens), f32),
            pltpu.VMEM((tokens, heads * head_dim), bf),
            pltpu.VMEM((tokens, depth), bf),
            pltpu.VMEM((tokens, depth), f32),
            pltpu.VMEM((tokens, cols), bf),
            dma((max(heads, depth // head_dim),)),
            dma((2, 3)),
            dma((2, 2)),
            dma((2,)),
        ],
        compiler_params=pltpu.CompilerParams(vmem_limit_bytes=VMEM_LIMIT),
        name="rest",
    )(o, x, g_attn, g_mlp, wq, wo, wg, wu, wd, k_all, v_all)


def solution(mesh):
    n_sp = mesh.shape["sp"]
    row_spec = P(("dp", "sp"), None)
    in_specs = (row_spec,) + (P(),) * 10

    def local_block(x, g_kv, w_k, w_v, g_attn, w_q, w_o, g_mlp, w_gate, w_up, w_down):
        depth = x.shape[1]
        wk = w_k.transpose(1, 0, 2)
        wv = w_v.transpose(1, 0, 2)
        wq = w_q.transpose(0, 2, 1, 3)
        wo = w_o.reshape(w_o.shape[0], -1, depth)
        k_all, v_all, o = gather_attend(
            n_sp, x, g_kv, g_attn, wk, wv, wq)
        h = rest(n_sp, o, x, g_attn, g_mlp, wq, wo, w_gate, w_up, w_down, k_all, v_all)
        return h

    return jax.shard_map(local_block, mesh=mesh, in_specs=in_specs, out_specs=row_spec, check_vma=False)
```
